32 devices in a mesh: gz: 8 (over z, x), gy: 4 (over y, core).
Axes of the slice: x: 2, y: 2, z: 4, core: 2. Of those that a mesh axis runs over, the one named last changes fastest.
Arguments:
- source: float32 [32, 64, 512], P('gz', 'gy'), may hold values from -8 to 8
- conduct: float32 [32, 64, 512], P('gz', 'gy'), may hold values from 0.5 to 4
Outputs:
- adjoint: float32 [32, 64, 512], P('gz', 'gy')
- residual: float32 [32, 64, 512], P('gz', 'gy')
The draws below stay inside these ranges and needn't reach their ends.
All inputs are finite; a program needn't handle non-finite values.
Results may differ from the reference program's by a relative error of at most 0.0003.
Values sent between devices are 32-bit elements; how exact they have to be, the bound alone decides.
A program may use at most 64 MiB of HBM per device.

```python
import math
import jax
import jax.numpy as jnp

NX = 512
DEGREE = 3
COARSE_DEGREE = 4
CYCLES = 2
NZ = 32
NY = 64


def levels(stream_key, dims, split, least, largest):
    gain, own = 1.0, jax.random.fold_in(stream_key, 6)
    for axis_at, shards_of in split:
        heights = jnp.exp(jax.random.uniform(jax.random.fold_in(own, axis_at), (shards_of,), jnp.float32, least / len(split), largest / len(split)))
        gain = gain * jnp.repeat(heights, dims[axis_at] // shards_of).reshape([-1 if axis == axis_at else 1 for axis in range(len(dims))])
    return gain


def normal_values(stream_key, extent, deviation, most, cuts=(), kind=jnp.bfloat16):
    factor_of = levels(stream_key, extent, cuts, -0.22, 0.18) if cuts else 1.0
    entries = jax.random.normal(stream_key, extent, jnp.float32) * deviation * factor_of
    return jnp.minimum(jnp.maximum(entries, -most), most).astype(kind)


def setup_inputs(seed: int = 0) -> dict:
    splits = jax.random.split(jax.random.key(seed), 3)
    source = normal_values(splits[0], (NZ, NY, NX), 1.0, 8.0, ((0, 8), (1, 4)), jnp.float32)
    conduct = jnp.clip(jnp.exp(math.log(4.0) - 2.0794415 * jax.random.uniform(splits[1], (NZ, NY, NX), jnp.float32) ** levels(splits[1], (NZ, NY, NX), ((0, 8), (1, 4)), -0.2, 0.2)), 0.5, 4.0)
    return {"source": source, "conduct": conduct}


cheb_low = 0.3
cheb_high = 1.9
heat_step = 4.0


def apply_level(field, conduct, scale):
    w = conduct * field
    beside = jnp.roll(w, -1, 0) + jnp.roll(w, 1, 0)
    beside = beside + jnp.roll(w, -1, 1) + jnp.roll(w, 1, 1)
    padded = jnp.pad(w, ((0, 0), (0, 0), (1, 1)))
    beside = beside + padded[:, :, 2:] + padded[:, :, :-2]
    return field + scale * (6.0 * w - beside)


def restrict(field):
    z, y, x = field.shape
    return field.reshape(z // 2, 2, y // 2, 2, x // 2, 2).mean(axis=(1, 3, 5))


def prolong(field):
    return jnp.repeat(jnp.repeat(jnp.repeat(field, 2, 0), 2, 1), 2, 2)


def smooth(apply_fn, rhs, start, inv_diag, steps):
    theta = (cheb_high + cheb_low) / 2.0
    delta = (cheb_high - cheb_low) / 2.0
    sigma = theta / delta
    rho = 1.0 / sigma
    if start is None:
        correct = inv_diag * rhs
        change = correct / theta
        field = change
    else:
        correct = inv_diag * (rhs - apply_fn(start))
        change = correct / theta
        field = start + change
    for step in range(steps - 1):
        rho_next = 1.0 / (2.0 * sigma - rho)
        correct = inv_diag * (rhs - apply_fn(field))
        change = rho_next * rho * change + (2.0 * rho_next / delta) * correct
        field = field + change
        rho = rho_next
    return field


def vcycle(rhs, conducts, scales):
    ops = [partial_apply(conducts[i], scales[i]) for i in range(3)]
    diags = [1.0 / (1.0 + 6.0 * scales[i] * conducts[i]) for i in range(3)]
    fine = smooth(ops[0], rhs, None, diags[0], DEGREE)
    rhs_mid = restrict(rhs - ops[0](fine))
    middle = smooth(ops[1], rhs_mid, None, diags[1], DEGREE)
    rhs_low = restrict(rhs_mid - ops[1](middle))
    lowest = smooth(ops[2], rhs_low, None, diags[2], COARSE_DEGREE)
    middle = smooth(ops[1], rhs_mid, middle + prolong(lowest), diags[1], DEGREE)
    fine = smooth(ops[0], rhs, fine + prolong(middle), diags[0], DEGREE)
    return fine


def partial_apply(conduct, scale):
    def inner(field):
        return apply_level(field, conduct, scale)
    return inner


def reference(source, conduct):
    mid_cond = restrict(conduct)
    conducts = [conduct, mid_cond, restrict(mid_cond)]
    scales = [heat_step, heat_step / 4.0, heat_step / 16.0]
    adjoint = jnp.zeros_like(source)
    remain = source
    for cycle in range(CYCLES):
        adjoint = adjoint + vcycle(remain, conducts, scales)
        remain = source - apply_level(adjoint, conduct, heat_step)
    return adjoint, remain
```

```python
import functools

import jax
import jax.numpy as jnp
from jax import lax
from jax.experimental import pallas as pl
from jax.experimental.pallas import tpu as pltpu
from jax.sharding import PartitionSpec as P

DEGREE = 3
COARSE_DEGREE = 4
CYCLES = 2

cheb_low = 0.3
cheb_high = 1.9
heat_step = 4.0
SCALES = (heat_step, heat_step / 4.0, heat_step / 16.0)

HALO = 4
ROWS = 8
MID_REACH = 15
MESH = pl.DeviceIdType.MESH
HIGH = lax.Precision.HIGHEST


def coefficients(steps):
    theta = (cheb_high + cheb_low) / 2.0
    delta = (cheb_high - cheb_low) / 2.0
    sigma = theta / delta
    rho = 1.0 / sigma
    pairs = [(0.0, 1.0 / theta)]
    for _ in range(steps - 1):
        rho_next = 1.0 / (2.0 * sigma - rho)
        pairs.append((rho_next * rho, 2.0 * rho_next / delta))
        rho = rho_next
    return pairs


def window(devices, cells, even):
    reach = -(-MID_REACH // cells)
    count = 2 * reach + 1
    if even:
        count += count % 2
    if count >= devices:
        count = devices
    ahead = count // 2
    return [s if s <= ahead else s - count for s in range(count)]


def select(shape, pick, value):
    rows = lax.broadcasted_iota(jnp.int32, shape, 0)
    columns = lax.broadcasted_iota(jnp.int32, shape, 1)
    return jnp.where(pick(rows, columns), value, 0.0).astype(jnp.float32)


def dot(a, b):
    return jnp.dot(a, b, precision=HIGH, preferred_element_type=jnp.float32)


def narrow(value):
    pairs = select((256, 128), lambda r, c: (r >> 1) == c, 1.0)
    parts = [dot(value[:, i : i + 256], pairs) for i in range(0, value.shape[1], 256)]
    return parts[0] if len(parts) == 1 else jnp.concatenate(parts, axis=1)


def widen(value):
    pairs = select((128, 256), lambda r, c: r == (c >> 1), 1.0)
    parts = [dot(value[:, i : i + 128], pairs) for i in range(0, value.shape[1], 128)]
    return parts[0] if len(parts) == 1 else jnp.concatenate(parts, axis=1)


def beside_of(w, plane):
    planes = w.shape[0]
    here = w[plane]
    rows, columns = here.shape
    lane = lax.broadcasted_iota(jnp.int32, here.shape, 1)
    total = w[lax.rem(plane + 1, planes)] + w[lax.rem(plane + planes - 1, planes)]
    total = total + pltpu.roll(here, 1, 0) + pltpu.roll(here, rows - 1, 0)
    left = jnp.where(lane == 0, 0.0, pltpu.roll(here, 1, 1))
    right = jnp.where(lane == columns - 1, 0.0, pltpu.roll(here, columns - 1, 1))
    return here, total + left + right


def over(planes, own, margin, body):
    if margin is None:
        first, count = 0, planes
    else:
        first, count = planes - margin, own + 2 * margin

    def step(i, carry):
        body(lax.rem(i + first, planes))
        return carry

    lax.fori_loop(0, count, step, 0)


class Level:
    def __init__(self, k, inverse, x, d, w, own, scale):
        self.k, self.inverse, self.x, self.d, self.w = k, inverse, x, d, w
        self.own, self.scale, self.planes = own, scale, k.shape[0]

    def run(self, margin, body):
        over(self.planes, self.own, margin, body)

    def prepare(self, margin):
        def body(p):
            self.inverse[p] = 1.0 / (1.0 + 6.0 * self.scale * self.k[p])

        self.run(margin, body)

    def smooth(self, f, steps, margins, zero):
        now = 0
        for step, (keep, gain) in enumerate(coefficients(steps)):
            old, new = self.w[now], self.w[1 - now]

            def body(p, step=step, keep=keep, gain=gain, old=old, new=new):
                if step == 0 and zero:
                    change = gain * (self.inverse[p] * f[p])
                    field = change
                else:
                    here, beside = beside_of(old, p)
                    field = self.x[p]
                    image = field + self.scale * (6.0 * here - beside)
                    change = gain * (self.inverse[p] * (f[p] - image))
                    if step:
                        change = keep * self.d[p] + change
                    field = field + change
                self.d[p] = change
                self.x[p] = field
                new[p] = self.k[p] * field

            self.run(margins[step], body)
            now = 1 - now
        return self.w[now]

    def residual(self, f, x, w, out, margin):
        def body(p):
            here, beside = beside_of(w, p)
            out[p] = f[p] - (x[p] + self.scale * (6.0 * here - beside))

        self.run(margin, body)


def kernel(sizes, z_window, y_window, source, conduct, adjoint, residual,
           src, k0, inv0, x0, d0, wa0, wb0, r0, r1, early, adj, late,
           k1, inv1, x1, d1, wa1, wb1, t1, f1a, f1b,
           k2, inv2, x2, d2, wa2, wb2, f2, halo_send, halo_recv, mid_send, mid_recv):
    gz, gy = sizes
    own_z, own_y, _ = source.shape
    mz, my = own_z // 2, own_y // 2
    me_z, me_y = lax.axis_index("gz"), lax.axis_index("gy")
    at_z = lambda o: (lax.rem(me_z + o + gz, gz), me_y)
    at_y = lambda o: (me_z, lax.rem(me_y + o + gy, gy))

    barrier = pltpu.get_barrier_semaphore()
    greet_z = sorted({o % gz for o in z_window} | {-o % gz for o in z_window})[1:]
    greet_y = sorted({o % gy for o in y_window} | {-o % gy for o in y_window})[1:]
    for o in greet_z:
        pl.semaphore_signal(barrier, inc=1, device_id=at_z(o), device_id_type=MESH)
    for o in greet_y:
        pl.semaphore_signal(barrier, inc=1, device_id=at_y(o), device_id_type=MESH)
    pl.semaphore_wait(barrier, len(greet_z) + len(greet_y))

    started = []

    def send(from_ref, to_ref, send_sem, recv_sem, device):
        copy = pltpu.make_async_remote_copy(
            src_ref=from_ref, dst_ref=to_ref, send_sem=send_sem, recv_sem=recv_sem,
            device_id=device, device_id_type=MESH)
        copy.start()
        started.append(copy)
        return copy

    zs = 3 * own_z
    ys = own_y + 2 * ROWS

    class Halo:
        def __init__(self, number, own, held, depth):
            self.number, self.held, self.depth, self.count = number, held, depth, 0
            self.z = [
                self.put(own.at[pl.ds(own_z - depth, depth)],
                         held.at[pl.ds(zs - depth, depth), pl.ds(0, own_y)], at_z(1)),
                self.put(own.at[pl.ds(0, depth)],
                         held.at[pl.ds(own_z, depth), pl.ds(0, own_y)], at_z(-1)),
            ]
            self.y = self.rows(own, 0, own_z)

        def put(self, from_ref, to_ref, device):
            i = self.count
            self.count += 1
            return send(from_ref, to_ref, halo_send.at[self.number, i],
                        halo_recv.at[self.number, i], device)

        def rows(self, own, first, count):
            planes = pl.ds(first, count)
            return [
                self.put(own.at[planes, pl.ds(own_y - ROWS, ROWS)],
                         self.held.at[planes, pl.ds(own_y + ROWS, ROWS)], at_y(1)),
                self.put(own.at[planes, pl.ds(0, ROWS)],
                         self.held.at[planes, pl.ds(own_y, ROWS)], at_y(-1)),
            ]

        def forward(self):
            self.z[0].wait_recv()
            self.y += self.rows(self.held, zs - self.depth, self.depth)
            self.z[1].wait_recv()
            self.y += self.rows(self.held, own_z, self.depth)

        def wait(self):
            for copy in self.y:
                copy.wait_recv()

    near = sorted(range(len(z_window)), key=lambda s: abs(z_window[s]))
    wide_y = len(y_window)

    class Gather:
        def __init__(self, number, held):
            self.number, self.held = number, held
            self.z = {}
            for s in near[1:][::-1]:
                self.z[s] = send(
                    self.block(0, 0), self.block(s, 0), mid_send.at[number, s * wide_y],
                    mid_recv.at[number, s * wide_y], at_z(-z_window[s]))
            self.y = []
            self.spread(0)

        def block(self, s, t):
            return self.held.at[pl.ds(s * mz, mz), pl.ds(t * my, my)]

        def spread(self, s):
            for t in range(1, wide_y):
                self.y.append(send(
                    self.block(s, 0), self.block(s, t), mid_send.at[self.number, s * wide_y + t],
                    mid_recv.at[self.number, s * wide_y + t], at_y(-y_window[t])))

        def forward(self):
            for s in near[1:]:
                self.z[s].wait_recv()
                self.spread(s)

        def wait(self):
            for copy in self.y:
                copy.wait_recv()

    def coarsen(fine, coarse, planes, rows):
        lines = select((rows // 2, rows), lambda r, c: r == (c >> 1), 0.125)

        def body(p, carry):
            both = fine[2 * p, pl.ds(0, rows)] + fine[2 * p + 1, pl.ds(0, rows)]
            coarse[p, pl.ds(0, rows // 2)] = narrow(dot(lines, both))
            return carry

        lax.fori_loop(0, planes, body, 0)

    fine = Level(k0, inv0, x0, d0, (wa0, wb0), own_z, SCALES[0])
    middle = Level(k1, inv1, x1, d1, (wa1, wb1), None, SCALES[1])
    low = Level(k2, inv2, x2, d2, (wa2, wb2), None, SCALES[2])
    mid_planes, mid_rows, low_planes = k1.shape[0], k1.shape[1], k2.shape[0]

    source_halo = Halo(0, source, src, HALO - 1)
    conduct_halo = Halo(1, conduct, k0, HALO)
    src[pl.ds(0, own_z), pl.ds(0, own_y)] = source[...]
    k0[pl.ds(0, own_z), pl.ds(0, own_y)] = conduct[...]
    coarsen(k0, k1, mz, own_y)
    conduct_mid = Gather(0, k1)
    source_halo.forward()
    conduct_halo.forward()
    conduct_mid.forward()
    source_halo.wait()
    conduct_halo.wait()
    fine.prepare(HALO)

    def down(f, f1, number, held, halo_number, depth):
        w = fine.smooth(f, DEGREE, (3, 2, 1), True)
        held[pl.ds(0, own_z), pl.ds(0, own_y)] = x0[pl.ds(0, own_z), pl.ds(0, own_y)]
        fine.residual(f, x0, w, r0, 0)
        coarsen(r0, f1, mz, own_y)
        gather = Gather(number, f1)
        halo = Halo(halo_number, held.at[pl.ds(0, own_z), pl.ds(0, own_y)], held, depth)
        gather.forward()
        halo.forward()
        return gather, halo

    def solve(f1):
        w = middle.smooth(f1, DEGREE, (None,) * DEGREE, True)
        middle.residual(f1, x1, w, t1, None)
        coarsen(t1, f2, low_planes, mid_rows)
        low.smooth(f2, COARSE_DEGREE, (None,) * COARSE_DEGREE, True)
        lines = select((mid_rows, mid_rows // 2), lambda r, c: (r >> 1) == c, 1.0)

        def body(p, carry):
            add = widen(dot(lines, x2[p]))
            for half in range(2):
                field = x1[2 * p + half] + add
                x1[2 * p + half] = field
                wa1[2 * p + half] = k1[2 * p + half] * field
            return carry

        lax.fori_loop(0, low_planes, body, 0)
        middle.smooth(f1, DEGREE, (None,) * DEGREE, False)

    def up(f, held, margin):
        def pick(r, c):
            own = (r < own_y + ROWS) & ((r >> 1) == c)
            return own | ((r >= own_y + ROWS) & ((r >> 1) - (ys >> 1) + mid_rows == c))

        lines = select((ys, mid_rows), pick, 1.0)
        pairs = zs // 2
        sides = (margin + 1) // 2

        def body(i, carry):
            pair = lax.rem(i + pairs - sides, pairs)
            late_pair = (pair >= own_z).astype(jnp.int32)
            add = widen(dot(lines, x1[pair + late_pair * (mid_planes - pairs)]))
            for half in range(2):
                p = 2 * pair + half
                field = held[p] + add
                x0[p] = field
                wa0[p] = k0[p] * field
            return carry

        lax.fori_loop(0, mz + 2 * sides, body, 0)
        return fine.smooth(f, DEGREE, (margin - 1, margin - 2, margin - 3), False)

    gather, halo = down(src, f1a, 1, early, 2, HALO - 1)
    conduct_mid.wait()
    middle.prepare(None)
    coarsen(k1, k2, low_planes, mid_rows)
    low.prepare(None)
    gather.wait()
    solve(f1a)
    halo.wait()
    up(src, early, HALO - 1)
    adj[pl.ds(0, own_z), pl.ds(0, own_y)] = x0[pl.ds(0, own_z), pl.ds(0, own_y)]
    halo = Halo(3, adj.at[pl.ds(0, own_z), pl.ds(0, own_y)], adj, HALO)
    halo.forward()
    halo.wait()

    def weigh(p):
        wa0[p] = k0[p] * adj[p]

    fine.run(HALO, weigh)
    fine.residual(src, adj, wa0, r1, HALO - 1)

    gather, halo = down(r1, f1b, 2, late, 4, HALO)
    gather.wait()
    solve(f1b)
    halo.wait()
    up(r1, late, HALO)

    def finish(p):
        field = adj[p] + x0[p]
        x0[p] = field
        wa0[p] = k0[p] * field

    fine.run(1, finish)
    fine.residual(src, x0, wa0, r0, 0)
    adjoint[...] = x0[pl.ds(0, own_z), pl.ds(0, own_y)]
    residual[...] = r0[pl.ds(0, own_z), pl.ds(0, own_y)]
    for copy in started:
        copy.wait_send()


def local(sizes, source, conduct):
    own_z, own_y, nx = source.shape
    z_window = window(sizes[0], own_z // 2, False)
    y_window = window(sizes[1], own_y // 2, True)
    fine = (3 * own_z, own_y + 2 * ROWS, nx)
    mid = (len(z_window) * own_z // 2, len(y_window) * own_y // 2, nx // 2)
    low = tuple(n // 2 for n in mid)
    slots = len(z_window) * len(y_window)
    vmem = lambda shape, count: [pltpu.VMEM(shape, jnp.float32)] * count
    whole = pl.BlockSpec(memory_space=pltpu.VMEM)
    return pl.pallas_call(
        functools.partial(kernel, sizes, z_window, y_window),
        out_shape=[jax.ShapeDtypeStruct(source.shape, jnp.float32)] * 2,
        in_specs=[whole] * 2,
        out_specs=[whole] * 2,
        scratch_shapes=vmem(fine, 12) + vmem(mid, 9) + vmem(low, 7) + [
            pltpu.SemaphoreType.DMA((5, 8)),
            pltpu.SemaphoreType.DMA((5, 8)),
            pltpu.SemaphoreType.DMA((3, slots)),
            pltpu.SemaphoreType.DMA((3, slots)),
        ],
        compiler_params=pltpu.CompilerParams(
            collective_id=0, has_side_effects=True, vmem_limit_bytes=56 * 1024 * 1024
        ),
    )(source, conduct)


def solution(mesh):
    spec = P("gz", "gy", None)
    sizes = (mesh.shape["gz"], mesh.shape["gy"])
    return jax.shard_map(
        functools.partial(local, sizes),
        mesh=mesh,
        in_specs=(spec, spec),
        out_specs=(spec, spec),
        check_vma=False,
    )
```

```python
import functools

import jax
import jax.numpy as jnp
from jax import lax
from jax.experimental import pallas as pl
from jax.experimental.pallas import tpu as pltpu
from jax.sharding import PartitionSpec as P

DEGREE = 3
COARSE_DEGREE = 4
CYCLES = 2

cheb_low = 0.3
cheb_high = 1.9
heat_step = 4.0
SCALES = (heat_step, heat_step / 4.0, heat_step / 16.0)

HALO = 4
ROWS = 8
MID_REACH = 15
MESH = pl.DeviceIdType.MESH
LANES = 128


def coefficients(steps):
    theta = (cheb_high + cheb_low) / 2.0
    delta = (cheb_high - cheb_low) / 2.0
    sigma = theta / delta
    rho = 1.0 / sigma
    pairs = [(0.0, 1.0 / theta)]
    for _ in range(steps - 1):
        rho_next = 1.0 / (2.0 * sigma - rho)
        pairs.append((rho_next * rho, 2.0 * rho_next / delta))
        rho = rho_next
    return pairs


def window(devices, cells, even):
    reach = -(-MID_REACH // cells)
    count = 2 * reach + 1
    if even:
        count += count % 2
    if count >= devices:
        count = devices
    ahead = count // 2
    return [s if s <= ahead else s - count for s in range(count)]


def select(shape, pick, value):
    rows = lax.broadcasted_iota(jnp.int32, shape, 0)
    columns = lax.broadcasted_iota(jnp.int32, shape, 1)
    return jnp.where(pick(rows, columns), value, 0.0).astype(jnp.bfloat16)


def parts_of(value):
    parts = []
    for _ in range(3):
        parts.append(value.astype(jnp.bfloat16))
        value = value - parts[-1].astype(jnp.float32)
    return parts


def dot(a, b):
    return jnp.dot(a, b, preferred_element_type=jnp.float32)


def pick_rows(lines, value):
    high, middle, low = (dot(lines, part) for part in parts_of(value))
    return high + (middle + low)


def pick_columns(value, columns):
    high, middle, low = (dot(part, columns) for part in parts_of(value))
    return high + (middle + low)


def chunks(value):
    return [value[:, i : i + LANES] for i in range(0, value.shape[1], LANES)]


def join(parts):
    return parts[0] if len(parts) == 1 else jnp.concatenate(parts, axis=1)


def narrow(value):
    parts = chunks(value)
    return join([parts[i] + parts[i + 1] for i in range(0, len(parts), 2)])


def widen(value):
    return join([part for part in chunks(value) for _ in range(2)])


def along_x(here):
    parts = chunks(here)
    lane = lax.broadcasted_iota(jnp.int32, parts[0].shape, 1)
    first = jnp.where(lane == 0, 0.0, pltpu.roll(parts[-1], 1, 1))
    last = jnp.where(lane == LANES - 1, 0.0, pltpu.roll(parts[0], LANES - 1, 1))
    around = [first] + parts + [last]
    return join([around[j] + around[j + 2] for j in range(len(parts))])


def beside_of(w, plane):
    planes = w.shape[0]
    here = w[plane]
    rows = here.shape[0]
    total = w[lax.rem(plane + 1, planes)] + w[lax.rem(plane + planes - 1, planes)]
    total = total + pltpu.roll(here, 1, 0) + pltpu.roll(here, rows - 1, 0)
    return here, total + along_x(here)


def unrolled(count):
    return 4 if count % 4 == 0 else 2 if count % 2 == 0 else 1


def over(planes, own, margin, body):
    if margin is None:
        first, count = 0, planes
    else:
        first, count = planes - margin, own + 2 * margin

    def step(i, carry):
        body(lax.rem(i + first, planes))
        return carry

    lax.fori_loop(0, count, step, 0, unroll=unrolled(count))


class Level:
    def __init__(self, k, inverse, x, d, w, own, scale):
        self.k, self.inverse, self.x, self.d, self.w = k, inverse, x, d, w
        self.own, self.scale, self.planes = own, scale, k.shape[0]

    def run(self, margin, body):
        over(self.planes, self.own, margin, body)

    def prepare(self, margin):
        def body(p):
            self.inverse[p] = 1.0 / (1.0 + 6.0 * self.scale * self.k[p])

        self.run(margin, body)

    def smooth(self, f, steps, margins, zero):
        now = 0
        for step, (keep, gain) in enumerate(coefficients(steps)):
            old, new = self.w[now], self.w[1 - now]

            def body(p, step=step, keep=keep, gain=gain, old=old, new=new):
                if step == 0 and zero:
                    change = gain * (self.inverse[p] * f[p])
                    field = change
                else:
                    here, beside = beside_of(old, p)
                    field = self.x[p]
                    image = field + self.scale * (6.0 * here - beside)
                    change = gain * (self.inverse[p] * (f[p] - image))
                    if step:
                        change = keep * self.d[p] + change
                    field = field + change
                self.d[p] = change
                self.x[p] = field
                new[p] = self.k[p] * field

            self.run(margins[step], body)
            now = 1 - now
        return self.w[now]

    def residual(self, f, x, w, out, margin):
        def body(p):
            here, beside = beside_of(w, p)
            out[p] = f[p] - (x[p] + self.scale * (6.0 * here - beside))

        self.run(margin, body)


def kernel(sizes, z_window, y_window, source, conduct, adjoint, residual,
           src, k0, inv0, x0, d0, wa0, wb0, r0, r1, early, adj, late,
           k1, inv1, x1, d1, wa1, wb1, t1, f1a, f1b,
           k2, inv2, x2, d2, wa2, wb2, f2, halo_send, halo_recv, mid_send, mid_recv):
    gz, gy = sizes
    own_z, own_y, _ = source.shape
    mz, my = own_z // 2, own_y // 2
    me_z, me_y = lax.axis_index("gz"), lax.axis_index("gy")
    at_z = lambda o: (lax.rem(me_z + o + gz, gz), me_y)
    at_y = lambda o: (me_z, lax.rem(me_y + o + gy, gy))

    barrier = pltpu.get_barrier_semaphore()
    greet_z = sorted({o % gz for o in z_window} | {-o % gz for o in z_window})[1:]
    greet_y = sorted({o % gy for o in y_window} | {-o % gy for o in y_window})[1:]
    for o in greet_z:
        pl.semaphore_signal(barrier, inc=1, device_id=at_z(o), device_id_type=MESH)
    for o in greet_y:
        pl.semaphore_signal(barrier, inc=1, device_id=at_y(o), device_id_type=MESH)
    pl.semaphore_wait(barrier, len(greet_z) + len(greet_y))

    started = []

    def send(from_ref, to_ref, send_sem, recv_sem, device):
        copy = pltpu.make_async_remote_copy(
            src_ref=from_ref, dst_ref=to_ref, send_sem=send_sem, recv_sem=recv_sem,
            device_id=device, device_id_type=MESH)
        copy.start()
        started.append(copy)
        return copy

    zs = 3 * own_z
    ys = own_y + 2 * ROWS

    class Halo:
        def __init__(self, number, own, held, depth):
            self.number, self.held, self.depth, self.count = number, held, depth, 0
            self.z = [
                self.put(own.at[pl.ds(own_z - depth, depth)],
                         held.at[pl.ds(zs - depth, depth), pl.ds(0, own_y)], at_z(1)),
                self.put(own.at[pl.ds(0, depth)],
                         held.at[pl.ds(own_z, depth), pl.ds(0, own_y)], at_z(-1)),
            ]
            self.y = self.rows(own, 0, own_z)

        def put(self, from_ref, to_ref, device):
            i = self.count
            self.count += 1
            return send(from_ref, to_ref, halo_send.at[self.number, i],
                        halo_recv.at[self.number, i], device)

        def rows(self, own, first, count):
            planes = pl.ds(first, count)
            return [
                self.put(own.at[planes, pl.ds(own_y - ROWS, ROWS)],
                         self.held.at[planes, pl.ds(own_y + ROWS, ROWS)], at_y(1)),
                self.put(own.at[planes, pl.ds(0, ROWS)],
                         self.held.at[planes, pl.ds(own_y, ROWS)], at_y(-1)),
            ]

        def forward(self):
            self.z[0].wait_recv()
            self.y += self.rows(self.held, zs - self.depth, self.depth)
            self.z[1].wait_recv()
            self.y += self.rows(self.held, own_z, self.depth)

        def wait(self):
            for copy in self.y:
                copy.wait_recv()

    near = sorted(range(len(z_window)), key=lambda s: abs(z_window[s]))
    wide_y = len(y_window)

    class Gather:
        def __init__(self, number, held):
            self.number, self.held = number, held
            self.z = {}
            for s in near[1:][::-1]:
                self.z[s] = send(
                    self.block(0, 0), self.block(s, 0), mid_send.at[number, s * wide_y],
                    mid_recv.at[number, s * wide_y], at_z(-z_window[s]))
            self.y = []
            self.spread(0)

        def block(self, s, t):
            return self.held.at[pl.ds(s * mz, mz), pl.ds(t * my, my)]

        def spread(self, s):
            for t in range(1, wide_y):
                self.y.append(send(
                    self.block(s, 0), self.block(s, t), mid_send.at[self.number, s * wide_y + t],
                    mid_recv.at[self.number, s * wide_y + t], at_y(-y_window[t])))

        def forward(self):
            for s in near[1:]:
                self.z[s].wait_recv()
                self.spread(s)

        def wait(self):
            for copy in self.y:
                copy.wait_recv()

    def coarsen(fine, coarse, planes, rows):
        lines = select((rows // 2, rows), lambda r, c: r == (c >> 1), 0.125)

        def body(p, carry):
            both = fine[2 * p, pl.ds(0, rows)] + fine[2 * p + 1, pl.ds(0, rows)]
            coarse[p, pl.ds(0, rows // 2)] = pick_rows(lines, narrow(both))
            return carry

        lax.fori_loop(0, planes, body, 0, unroll=unrolled(planes))

    fine = Level(k0, inv0, x0, d0, (wa0, wb0), own_z, SCALES[0])
    middle = Level(k1, inv1, x1, d1, (wa1, wb1), None, SCALES[1])
    low = Level(k2, inv2, x2, d2, (wa2, wb2), None, SCALES[2])
    mid_planes, mid_rows, low_planes = k1.shape[0], k1.shape[1], k2.shape[0]

    nx = source.shape[2]
    share = nx // LANES

    def deal(r, c):
        return r == share * (c & (LANES - 1)) + c // LANES

    def own_of(ref):
        return ref.at[pl.ds(0, own_z), pl.ds(0, own_y)]

    def permuted(value, pick):
        columns = select((nx, nx), pick, 1.0)
        flat = value.reshape(own_z * own_y, nx)
        return pick_columns(flat, columns).reshape(own_z, own_y, nx)

    own_of(k0)[...] = permuted(conduct[...], deal)
    conduct_halo = Halo(1, own_of(k0), k0, HALO)
    own_of(src)[...] = permuted(source[...], deal)
    source_halo = Halo(0, own_of(src), src, HALO - 1)
    coarsen(k0, k1, mz, own_y)
    conduct_mid = Gather(0, k1)
    conduct_halo.forward()
    source_halo.forward()
    conduct_halo.wait()
    source_halo.wait()
    fine.prepare(HALO)
    conduct_mid.forward()

    def down(f, f1, number, held, halo_number, depth):
        w = fine.smooth(f, DEGREE, (3, 2, 1), True)
        held[pl.ds(0, own_z), pl.ds(0, own_y)] = x0[pl.ds(0, own_z), pl.ds(0, own_y)]
        fine.residual(f, x0, w, r0, 0)
        coarsen(r0, f1, mz, own_y)
        gather = Gather(number, f1)
        halo = Halo(halo_number, held.at[pl.ds(0, own_z), pl.ds(0, own_y)], held, depth)
        gather.forward()
        return gather, halo

    def solve(f1, halo):
        w = middle.smooth(f1, DEGREE, (None,) * DEGREE, True)
        halo.forward()
        middle.residual(f1, x1, w, t1, None)
        coarsen(t1, f2, low_planes, mid_rows)
        low.smooth(f2, COARSE_DEGREE, (None,) * COARSE_DEGREE, True)
        lines = select((mid_rows, mid_rows // 2), lambda r, c: (r >> 1) == c, 1.0)

        def body(p, carry):
            add = widen(pick_rows(lines, x2[p]))
            for half in range(2):
                field = x1[2 * p + half] + add
                x1[2 * p + half] = field
                wa1[2 * p + half] = k1[2 * p + half] * field
            return carry

        lax.fori_loop(0, low_planes, body, 0, unroll=unrolled(low_planes))
        middle.smooth(f1, DEGREE, (None,) * DEGREE, False)

    def up(f, held, margin):
        def pick(r, c):
            own = (r < own_y + ROWS) & ((r >> 1) == c)
            return own | ((r >= own_y + ROWS) & ((r >> 1) - (ys >> 1) + mid_rows == c))

        lines = select((ys, mid_rows), pick, 1.0)
        pairs = zs // 2
        sides = (margin + 1) // 2

        def body(i, carry):
            pair = lax.rem(i + pairs - sides, pairs)
            late_pair = (pair >= own_z).astype(jnp.int32)
            add = widen(pick_rows(lines, x1[pair + late_pair * (mid_planes - pairs)]))
            for half in range(2):
                p = 2 * pair + half
                field = held[p] + add
                x0[p] = field
                wa0[p] = k0[p] * field
            return carry

        lax.fori_loop(0, mz + 2 * sides, body, 0, unroll=unrolled(mz + 2 * sides))
        return fine.smooth(f, DEGREE, (margin - 1, margin - 2, margin - 3), False)

    gather, halo = down(src, f1a, 1, early, 2, HALO - 1)
    conduct_mid.wait()
    middle.prepare(None)
    coarsen(k1, k2, low_planes, mid_rows)
    low.prepare(None)
    gather.wait()
    solve(f1a, halo)
    halo.wait()
    up(src, early, HALO - 1)
    adj[pl.ds(0, own_z), pl.ds(0, own_y)] = x0[pl.ds(0, own_z), pl.ds(0, own_y)]
    halo = Halo(3, adj.at[pl.ds(0, own_z), pl.ds(0, own_y)], adj, HALO)
    halo.forward()
    halo.wait()

    def weigh(p):
        wa0[p] = k0[p] * adj[p]

    fine.run(HALO, weigh)
    fine.residual(src, adj, wa0, r1, HALO - 1)

    gather, halo = down(r1, f1b, 2, late, 4, HALO)
    gather.wait()
    solve(f1b, halo)
    halo.wait()
    up(r1, late, HALO)

    def finish(p):
        field = adj[p] + x0[p]
        x0[p] = field
        wa0[p] = k0[p] * field

    fine.run(1, finish)
    fine.residual(src, x0, wa0, r0, 0)
    for ref, out in ((x0, adjoint), (r0, residual)):
        out[...] = permuted(own_of(ref)[...], lambda r, c: deal(c, r))
    for copy in started:
        copy.wait_send()


def local(sizes, source, conduct):
    own_z, own_y, nx = source.shape
    z_window = window(sizes[0], own_z // 2, False)
    y_window = window(sizes[1], own_y // 2, True)
    fine = (3 * own_z, own_y + 2 * ROWS, nx)
    mid = (len(z_window) * own_z // 2, len(y_window) * own_y // 2, nx // 2)
    low = tuple(n // 2 for n in mid)
    slots = len(z_window) * len(y_window)
    vmem = lambda shape, count: [pltpu.VMEM(shape, jnp.float32)] * count
    whole = pl.BlockSpec(memory_space=pltpu.VMEM)
    return pl.pallas_call(
        functools.partial(kernel, sizes, z_window, y_window),
        out_shape=[jax.ShapeDtypeStruct(source.shape, jnp.float32)] * 2,
        in_specs=[whole] * 2,
        out_specs=[whole] * 2,
        scratch_shapes=vmem(fine, 12) + vmem(mid, 9) + vmem(low, 7) + [
            pltpu.SemaphoreType.DMA((5, 8)),
            pltpu.SemaphoreType.DMA((5, 8)),
            pltpu.SemaphoreType.DMA((3, slots)),
            pltpu.SemaphoreType.DMA((3, slots)),
        ],
        compiler_params=pltpu.CompilerParams(
            collective_id=0, has_side_effects=True, vmem_limit_bytes=56 * 1024 * 1024
        ),
    )(source, conduct)


def solution(mesh):
    spec = P("gz", "gy", None)
    sizes = (mesh.shape["gz"], mesh.shape["gy"])
    return jax.shard_map(
        functools.partial(local, sizes),
        mesh=mesh,
        in_specs=(spec, spec),
        out_specs=(spec, spec),
        check_vma=False,
    )
```
